32 devices in a mesh: dp: 8 (over z, core), tensor: 4 (over y, x).
Axes of the slice: x: 2, y: 2, z: 4, core: 2. Of those that a mesh axis runs over, the one named last changes fastest.
Arguments:
- tokens: bfloat16 [10240, 4096], P(('dp', 'tensor')), parts along dimension 0, may hold values from -6 to 6
- norm_gain: bfloat16 [4096], replicated, may hold values from 0.099609375 to 1.8984375
- query_weight: bfloat16 [4096, 8192], P(None, 'tensor'), may hold values from -0.09375 to 0.09375
- key_weight: bfloat16 [4096, 1024], P(None, 'tensor'), may hold values from -0.09375 to 0.09375
- value_weight: bfloat16 [4096, 1024], P(None, 'tensor'), may hold values from -0.09375 to 0.09375
- out_weight: bfloat16 [8192, 4096], P('tensor'), may hold values from -0.0625 to 0.0625
- past_cache: bfloat16 [1024, 64, 2, 1024], P('dp', None, None, 'tensor'), parts along dimension 0, may hold values from -320 to 320
- exponents: int32 [10240, 32], P('dp'), parts along dimension 0, may hold values from -11 to -7
Outputs:
- mixed: bfloat16 [10240, 4096], P(('dp', 'tensor')), parts along dimension 0
The draws below stay inside these ranges and needn't reach their ends.
There are 8 independent parts, one for each index of `dp`. The reference program is written for one: setup_inputs(seed, part) draws one part's arguments, and reference() takes and returns one part's arrays. A program takes and returns all parts, laid end to end along the dimension named above; an argument that names none is the same for every part. Nothing has to cross between parts.
All inputs are finite; a program needn't handle non-finite values.
Results may differ from the reference program's by a relative error of at most 0.012.
The reference program's roundings to bfloat16 on the way count: a program that leaves them out, or rounds other values in their place, can miss the bound.
Values may be sent and summed in bfloat16 or wider, within the bound.
A program may use at most 192 MiB of HBM per device.

```python
import jax
import jax.numpy as jnp
from jax import lax

D = 4096
QH = 64
KVH = 8
HD = 128
SEQS = 128
NEW = 10
CACHE = 64
QG = 128
ROWS = 1280
N_TENSOR = 4


def draw_past_cache(key, part):
    key_base = jax.random.fold_in(key, 11)
    shape_full = (SEQS, CACHE, 2, KVH * HD)
    values_out = jnp.clip(jax.random.normal(key_base, shape_full, jnp.float32), -4.0, 4.0)
    return values_out.astype(jnp.bfloat16)


def with_ends(array, key, least, top_value):
    longest = array.shape.index(max(array.shape))
    spots = []
    for shift in (0, 1):
        where = [jax.random.randint(jax.random.fold_in(key, axis), (), 0, length) for axis, length in enumerate(array.shape)]
        where[longest] = (where[longest] + shift) % array.shape[longest]
        spots.append(tuple(where))
    return array.at[spots[0]].set(least).at[spots[1]].set(top_value)


def block_scale(rng, dims, pieces, smallest, high):
    def one(dim, blocks):
        draws = jax.random.uniform(jax.random.fold_in(jax.random.fold_in(rng, 6), dim), (blocks,), jnp.float32, smallest / len(pieces), high / len(pieces))
        return jnp.repeat(jnp.exp(draws), dims[dim] // blocks).reshape((-1,) + (1,) * (len(dims) - dim - 1))

    gain = one(*pieces[0])
    for cut in pieces[1:]:
        gain = gain * one(*cut)
    return gain


def scatter_about(own_key, shape, width, limit, pieces=(), kind=jnp.bfloat16):
    gain = block_scale(own_key, shape, pieces, -0.22, 0.18) if pieces else 1.0
    result = jax.random.normal(own_key, shape, jnp.float32) * width * gain
    return jnp.minimum(jnp.maximum(result, -limit), limit).astype(kind)


def setup_inputs(seed: int = 0, part: int = 0) -> dict:
    streams_of = jax.random.split(jax.random.key(seed), 9)
    own_keys = jax.random.split(jax.random.fold_in(streams_of[8], part), 9)
    return {
        "tokens": scatter_about(own_keys[0], (ROWS, D), 1.0, 6.0, ((0, 4),)),
        "norm_gain": jnp.clip(1.0 + 0.18 * jax.random.normal(streams_of[1], (D,), jnp.float32), 0.099609375, 1.8984375).astype(jnp.bfloat16),
        "query_weight": scatter_about(streams_of[2], (D, QH * HD), D ** -0.5, 0.09375, ((1, 4),)),
        "key_weight": scatter_about(streams_of[3], (D, KVH * HD), D ** -0.5, 0.09375, ((1, 4),)),
        "value_weight": scatter_about(streams_of[4], (D, KVH * HD), D ** -0.5, 0.09375, ((1, 4),)),
        "out_weight": scatter_about(streams_of[5], (QH * HD, D), (QH * HD) ** -0.5, 0.0625, ((0, 4),)),
        "past_cache": draw_past_cache(jax.random.fold_in(jax.random.fold_in(streams_of[8], part), 71), part),
        "exponents": with_ends(jax.random.randint(own_keys[7], (ROWS, D // QG), -11, -6), jax.random.fold_in(own_keys[7], 1), -11, (-6) - 1).astype(jnp.int32),
    }


epsilon = 1e-05
theta_base = 500000.0

def rotate(matrix, heads):
    row_count = matrix.shape[0]
    half_dim = HD // 2
    positions = (jnp.arange(row_count, dtype=jnp.int32) % NEW + CACHE).astype(jnp.float32)
    frequency = theta_base ** (-(jnp.arange(half_dim, dtype=jnp.float32) * 2.0) / HD)
    angles = positions[:, None] * frequency[None, :]
    cosine = jnp.cos(angles)[:, None, :]
    sine_part = jnp.sin(angles)[:, None, :]
    shaped = matrix.reshape(row_count, heads, 2, half_dim)
    first = shaped[:, :, 0]
    second = shaped[:, :, 1]
    turned = jnp.stack([first * cosine - second * sine_part, second * cosine + first * sine_part], 2)
    return turned.reshape(row_count, heads * HD)

def attention(query, key_new, value_new, past_cache, kv_heads):
    row_count = query.shape[0]
    seq_count = row_count // NEW
    group_size = query.shape[1] // (kv_heads * HD)
    cache_len = past_cache.shape[1]
    query_heads = query.astype(jnp.float32).reshape(seq_count, NEW, kv_heads, group_size, HD)
    new_keys = key_new.astype(jnp.float32).reshape(seq_count, NEW, kv_heads, HD)
    new_values = value_new.astype(jnp.float32).reshape(seq_count, NEW, kv_heads, HD)
    cache_keys = past_cache[:, :, 0].astype(jnp.float32).reshape(seq_count, cache_len, kv_heads, HD)
    cache_values = past_cache[:, :, 1].astype(jnp.float32).reshape(seq_count, cache_len, kv_heads, HD)
    inv_root = 1.0 / HD ** 0.5
    cache_scores = jnp.einsum('stkgd,sckd->skgtc', query_heads, cache_keys) * inv_root
    new_scores = jnp.einsum('stkgd,sukd->skgtu', query_heads, new_keys) * inv_root
    causal = jnp.arange(NEW)[:, None] >= jnp.arange(NEW)[None, :]
    new_scores = jnp.where(causal, new_scores, -1e+30)
    row_max = jnp.maximum(cache_scores.max(-1), new_scores.max(-1))[..., None]
    cache_probs = jnp.exp(cache_scores - row_max)
    new_probs = jnp.exp(new_scores - row_max)
    denominator = (cache_probs.sum(-1) + new_probs.sum(-1))[..., None]
    cache_weights = (cache_probs / denominator).astype(jnp.bfloat16).astype(jnp.float32)
    new_weights = (new_probs / denominator).astype(jnp.bfloat16).astype(jnp.float32)
    combined = jnp.einsum('skgtc,sckd->stkgd', cache_weights, cache_values)
    combined = combined + jnp.einsum('skgtu,sukd->stkgd', new_weights, new_values)
    return combined.reshape(row_count, kv_heads * group_size * HD).astype(jnp.bfloat16)

def reference(tokens, norm_gain, query_weight, key_weight, value_weight, out_weight, past_cache, exponents):
    floats = tokens.astype(jnp.float32)
    normed = floats * lax.rsqrt(lax.optimization_barrier(jnp.mean(floats * floats, axis=-1, keepdims=True)) + epsilon)
    normed = (normed * norm_gain.astype(jnp.float32)).astype(jnp.bfloat16)
    query = rotate(jnp.dot(normed, query_weight, preferred_element_type=jnp.float32), QH).astype(jnp.bfloat16)
    key_new = rotate(jnp.dot(normed, key_weight, preferred_element_type=jnp.float32), KVH).astype(jnp.bfloat16)
    value_new = jnp.dot(normed, value_weight, preferred_element_type=jnp.float32).astype(jnp.bfloat16)
    attended = attention(query, key_new, value_new, past_cache, KVH)
    row_count = tokens.shape[0]
    groups = D // QG
    shrink = jnp.exp2(-exponents.astype(jnp.float32))[..., None]
    head_cols = QH * HD // N_TENSOR
    summed = jnp.zeros((row_count, groups, QG), jnp.float32)
    for rank in range(N_TENSOR):
        partial_value = jnp.dot(attended[:, rank * head_cols:(rank + 1) * head_cols], out_weight[rank * head_cols:(rank + 1) * head_cols], preferred_element_type=jnp.float32)
        scaled = jnp.clip(partial_value.reshape(row_count, groups, QG) * shrink, -127.0, 127.0)
        summed = summed + lax.optimization_barrier(scaled.astype(jnp.bfloat16)).astype(jnp.float32)
    restore = jnp.exp2(exponents.astype(jnp.float32))[..., None]
    layer_out = floats + (summed * restore).reshape(row_count, D)
    return layer_out.astype(jnp.bfloat16)
```

```python
import functools

import jax
import jax.numpy as jnp
import numpy as np
from jax import lax
from jax.experimental import pallas as pl
from jax.experimental.pallas import tpu as pltpu
from jax.sharding import PartitionSpec as P

HD = 128
NEW = 10
SEQ_BLOCK = 8
PIECE = SEQ_BLOCK * NEW
WIDTH = 512

epsilon = 1e-05
theta_base = 500000.0
MESH = pl.DeviceIdType.MESH


def rotary_tables(cache_len):
    half_dim = HD // 2
    positions = np.arange(PIECE) % NEW + cache_len
    frequency = theta_base ** (-(np.arange(half_dim) * 2.0) / HD)
    angles = positions[:, None] * frequency[None, :]
    cosine = np.cos(angles)
    sine_part = np.sin(angles)
    return (
        np.concatenate([cosine, cosine], 1).astype(np.float32),
        np.concatenate([-sine_part, sine_part], 1).astype(np.float32),
    )


def mask_table(cache_len):
    row = np.arange(PIECE)[:, None]
    cached = np.arange(SEQ_BLOCK * cache_len)[None, :]
    fresh = np.arange(PIECE)[None, :]
    in_cache = row // NEW == cached // cache_len
    in_new = (row // NEW == fresh // NEW) & (row % NEW >= fresh % NEW)
    return np.where(np.concatenate([in_cache, in_new], 1), 0.0, -1e30).astype(np.float32)


def ring_index(place, ranks):
    half = ranks // 2
    return jnp.where(place < half, place, half + ranks - 1 - place)


def layer_kernel(
    ranks,
    batches,
    tokens_ref,
    gain_ref,
    wq_ref,
    wk_ref,
    wv_ref,
    wo_ref,
    cache_ref,
    expo_ref,
    cos_ref,
    sin_ref,
    bias_ref,
    out_ref,
    slots,
    sums,
    wq,
    wk,
    wv,
    wo,
    heads,
    key_new,
    value_new,
    keys,
    values,
    raw,
    wide,
    expo,
    scale,
    local_sem,
    raw_sem,
    expo_sem,
    out_sem,
    gather_send,
    gather_recv,
    reduce_send,
    reduce_recv,
):
    unit = 2 * PIECE
    units = ranks * batches
    own_rows = unit * batches
    depth = slots.shape[2]
    q_cols = heads.shape[1]
    kv_heads = key_new.shape[1] // HD
    group = q_cols // (kv_heads * HD)
    cache_len = cache_ref.shape[1]
    cache_rows = SEQ_BLOCK * cache_len
    groups = expo_ref.shape[1]
    group_cols = depth // groups
    inv_root = 1.0 / HD**0.5

    me = lax.axis_index("tensor")
    place = ring_index(me, ranks)
    right = ring_index(lax.rem(place + 1, ranks), ranks)
    left = ring_index(lax.rem(place + ranks - 1, ranks), ranks)

    def piece_row(k, d):
        hop, batch = k // batches, k % batches
        source = lax.rem(place + ranks - hop, ranks) if d == 0 else lax.rem(place + hop, ranks)
        return ring_index(source, ranks) * own_rows + (2 * batch + d) * PIECE

    weight_copies = [
        pltpu.make_async_copy(src, dst, local_sem.at[i])
        for i, (src, dst) in enumerate(
            ((wq_ref, wq), (wk_ref, wk), (wv_ref, wv), (wo_ref, wo))
        )
    ]

    def token_copy(b, slot, sem):
        return pltpu.make_async_copy(
            tokens_ref.at[pl.ds(b * unit, unit), :], slots.at[slot], sem
        )

    def out_copy(b, slot):
        return pltpu.make_async_copy(
            slots.at[slot], out_ref.at[pl.ds(b * unit, unit), :], out_sem.at[b]
        )

    def raw_copy(k, d, kv):
        first = piece_row(k, d) // NEW
        return pltpu.make_async_copy(
            cache_ref.at[pl.ds(first, SEQ_BLOCK), :, :, pl.ds(kv * HD, HD)],
            raw.at[d * kv_heads + kv],
            raw_sem.at[d, kv],
        )

    def expo_copy(k, d):
        first = pl.multiple_of(piece_row(k, d), PIECE)
        return pltpu.make_async_copy(
            expo_ref.at[pl.ds(first, PIECE), :],
            expo.at[pl.ds(d * PIECE, PIECE), :],
            expo_sem.at[d],
        )

    def half(d):
        return pl.ds(d * PIECE, PIECE)

    def gather_copy(k, d):
        return pltpu.make_async_remote_copy(
            src_ref=slots.at[k + batches, half(d), :],
            dst_ref=slots.at[k + 2 * batches, half(d), :],
            send_sem=gather_send.at[k, d],
            recv_sem=gather_recv.at[k, d],
            device_id={"tensor": right if d == 0 else left},
            device_id_type=MESH,
        )

    def reduce_copy(k, d):
        return pltpu.make_async_remote_copy(
            src_ref=slots.at[k, half(d), :],
            dst_ref=sums.at[k - batches, half(d), :],
            send_sem=reduce_send.at[k - batches, d],
            recv_sem=reduce_recv.at[k - batches, d],
            device_id={"tensor": right if d == 0 else left},
            device_id_type=MESH,
        )

    for b in range(batches):
        token_copy(b, batches + b, out_sem.at[b]).start()
    for copy in weight_copies:
        copy.start()
    for d in range(2):
        for kv in range(kv_heads):
            raw_copy(0, d, kv).start()
        expo_copy(0, d).start()

    barrier = pltpu.get_barrier_semaphore()
    for neighbour in (left, right):
        pl.semaphore_signal(
            barrier, inc=1, device_id={"tensor": neighbour}, device_id_type=MESH
        )

    def norm(slot, d):
        def step(i, carry):
            rows = pl.ds(pl.multiple_of(d * PIECE + i * 16, 16), 16)
            floats = slots[slot, rows, :].astype(jnp.float32)
            normed = floats * lax.rsqrt(jnp.mean(floats * floats, axis=-1, keepdims=True) + epsilon)
            slots[slot, rows, :] = (normed * gain_ref[...].astype(jnp.float32)).astype(jnp.bfloat16)
            return carry

        lax.fori_loop(0, PIECE // 16, step, 0)

    token_copy(0, batches, out_sem.at[0]).wait()
    norm(batches, 0)
    norm(batches, 1)
    pl.semaphore_wait(barrier, 2)
    for d in range(2):
        gather_copy(0, d).start()
    for b in range(1, batches):
        token_copy(b, batches + b, out_sem.at[b]).wait()
        for d in range(2):
            norm(batches + b, d)
            gather_copy(b, d).start()

    def turn(block):
        cosine = cos_ref[...]
        sine_part = sin_ref[...]
        parts = []
        for d in range(2):
            turned = []
            for h in range(block.shape[1] // HD):
                head = block[d * PIECE : (d + 1) * PIECE, h * HD : (h + 1) * HD]
                turned.append(head * cosine + pltpu.roll(head, HD // 2, 1) * sine_part)
            parts.append(jnp.concatenate(turned, 1) if len(turned) > 1 else turned[0])
        return jnp.concatenate(parts, 0)

    def project(k):
        slot = k + batches
        width = min(WIDTH, q_cols)

        def tile(j, carry):
            cols = pl.ds(pl.multiple_of(j * width, width), width)
            query = jnp.dot(slots[slot], wq[:, cols], preferred_element_type=jnp.float32)
            heads[:, cols] = turn(query).astype(jnp.bfloat16)
            return carry

        lax.fori_loop(0, q_cols // width, tile, 0)
        key = jnp.dot(slots[slot], wk[...], preferred_element_type=jnp.float32)
        key_new[...] = turn(key).astype(jnp.bfloat16)
        value = jnp.dot(slots[slot], wv[...], preferred_element_type=jnp.float32)
        value_new[...] = value.astype(jnp.bfloat16)

    def attend(k, d):
        rows = half(d)
        bias = bias_ref[...]
        for kv in range(kv_heads):
            raw_copy(k, d, kv).wait()
            span = slice(kv * HD, (kv + 1) * HD)
            wide[...] = raw.at[d * kv_heads + kv].reshape(2 * cache_rows, HD)[...].astype(jnp.float32)
            keys[:cache_rows] = wide[pl.ds(0, cache_rows, 2), :].astype(jnp.bfloat16)
            values[:cache_rows] = wide[pl.ds(1, cache_rows, 2), :].astype(jnp.bfloat16)
            keys[cache_rows:] = key_new[rows, span]
            values[cache_rows:] = value_new[rows, span]

            @pl.when(k + 1 < units)
            def _():
                raw_copy(k + 1, d, kv).start()

            base = kv * group * HD
            query = jnp.concatenate(
                [heads[rows, base + g * HD : base + (g + 1) * HD] for g in range(group)], 0
            )
            scores = lax.dot_general(
                query, keys[...], (((1,), (1,)), ((), ())), preferred_element_type=jnp.float32
            )
            weights = []
            for g in range(group):
                part = scores[g * PIECE : (g + 1) * PIECE] * inv_root + bias
                probs = jnp.exp(part - jnp.max(part, axis=-1, keepdims=True))
                total = 1.0 / jnp.sum(probs, axis=-1, keepdims=True)
                weights.append((probs * total).astype(jnp.bfloat16))
            combined = jnp.dot(
                jnp.concatenate(weights, 0), values[...], preferred_element_type=jnp.float32
            ).astype(jnp.bfloat16)
            for g in range(group):
                heads[rows, base + g * HD : base + (g + 1) * HD] = combined[
                    g * PIECE : (g + 1) * PIECE
                ]

    def project_out(k):
        for d in range(2):
            expo_copy(k, d).wait()
        scale[:, :groups] = jnp.exp2(-expo[...].astype(jnp.float32))

        @pl.when(k + 1 < units)
        def _():
            for d in range(2):
                expo_copy(k + 1, d).start()

        per_tile = WIDTH // group_cols

        def tile(j, carry):
            cols = pl.ds(pl.multiple_of(j * WIDTH, WIDTH), WIDTH)
            partial_value = jnp.dot(heads[...], wo[:, cols], preferred_element_type=jnp.float32)
            shrink = scale[...]
            parts = []
            for i in range(per_tile):
                part = partial_value[:, i * group_cols : (i + 1) * group_cols]
                parts.append(jnp.clip(part * shrink[:, i : i + 1], -127.0, 127.0))
            slots[k, :, cols] = jnp.concatenate(parts, 1).astype(jnp.bfloat16)
            scale[...] = pltpu.roll(shrink, shrink.shape[1] - per_tile, 1)
            return carry

        lax.fori_loop(0, depth // WIDTH, tile, 0)

    def add_sums(k):
        def step(i, carry):
            rows = pl.ds(pl.multiple_of(i * 16, 16), 16)
            slots[k, rows, :] = (
                slots[k, rows, :].astype(jnp.float32)
                + sums[k - 2 * batches, rows, :].astype(jnp.float32)
            ).astype(jnp.bfloat16)
            return carry

        lax.fori_loop(0, unit // 16, step, 0)

    def body(k, carry):
        @pl.when(k >= units - batches)
        def _():
            for d in range(2):
                gather_copy(k - batches, d).wait_recv()

        @pl.when(k == 0)
        def _():
            for copy in weight_copies[:3]:
                copy.wait()

        project(k)
        for d in range(2):
            attend(k, d)

        @pl.when(k == 0)
        def _():
            weight_copies[3].wait()

        @pl.when(k >= batches)
        def _():
            for d in range(2):
                gather_copy(k - batches, d).wait_send()

        project_out(k)

        @pl.when(k + 2 * batches < units)
        def _():
            for d in range(2):
                gather_copy(k, d).wait_recv()
                gather_copy(k + batches, d).start()

        @pl.when(k >= 2 * batches)
        def _():
            for d in range(2):
                reduce_copy(k - batches, d).wait_recv()
            add_sums(k)

        @pl.when(k >= batches)
        def _():
            for d in range(2):
                reduce_copy(k, d).start()

        return carry

    lax.fori_loop(0, units, body, 0)

    for b in range(batches):
        token_copy(b, units + b, out_sem.at[b]).start()
    for b in range(batches):
        for d in range(2):
            expo_copy(b, d).start()
        token_copy(b, units + b, out_sem.at[b]).wait()
        for d in range(2):
            expo_copy(b, d).wait()
        scale[:, :groups] = jnp.exp2(expo[...].astype(jnp.float32))
        for d in range(2):
            reduce_copy(units - batches + b, d).wait_recv()

            def step(i, carry):
                rows = pl.ds(pl.multiple_of(d * PIECE + i * 16, 16), 16)
                for g in range(groups):
                    cols = slice(g * group_cols, (g + 1) * group_cols)
                    total = slots[b, rows, cols].astype(jnp.float32) + sums[
                        units - 2 * batches + b, rows, cols
                    ].astype(jnp.float32)
                    term = total * scale[rows, g : g + 1]
                    slots[units + b, rows, cols] = (
                        slots[units + b, rows, cols].astype(jnp.float32) + term
                    ).astype(jnp.bfloat16)
                return carry

            lax.fori_loop(0, PIECE // 16, step, 0)
        out_copy(b, units + b).start()
    for b in range(batches):
        out_copy(b, units + b).wait()

    def drain(k, carry):
        for d in range(2):
            reduce_copy(k, d).wait_send()
        return carry

    lax.fori_loop(batches, units, drain, 0)


def on_device(
    tokens, norm_gain, query_weight, key_weight, value_weight, out_weight, past_cache, exponents
):
    own_rows, depth = tokens.shape
    ranks = lax.axis_size("tensor")
    unit = 2 * PIECE
    batches = own_rows // unit
    units = ranks * batches
    q_cols = query_weight.shape[1]
    k_cols = key_weight.shape[1]
    kv_heads = k_cols // HD
    cache_len = past_cache.shape[1]
    cache_rows = SEQ_BLOCK * cache_len
    cosine, sine_part = rotary_tables(cache_len)
    bias = mask_table(cache_len)
    any_spec = pl.BlockSpec(memory_space=pl.ANY)
    vmem_spec = pl.BlockSpec(memory_space=pltpu.VMEM)
    bf16 = jnp.bfloat16
    dma = pltpu.SemaphoreType.DMA
    return pl.pallas_call(
        functools.partial(layer_kernel, ranks, batches),
        in_specs=[any_spec, vmem_spec] + [any_spec] * 6 + [vmem_spec] * 3,
        out_specs=any_spec,
        out_shape=jax.ShapeDtypeStruct(tokens.shape, bf16),
        scratch_shapes=[
            pltpu.VMEM((units + batches, unit, depth), bf16),
            pltpu.VMEM((units - batches, unit, depth), bf16),
            pltpu.VMEM((depth, q_cols), bf16),
            pltpu.VMEM((depth, k_cols), bf16),
            pltpu.VMEM((depth, k_cols), bf16),
            pltpu.VMEM((q_cols, depth), bf16),
            pltpu.VMEM((unit, q_cols), bf16),
            pltpu.VMEM((unit, k_cols), bf16),
            pltpu.VMEM((unit, k_cols), bf16),
            pltpu.VMEM((cache_rows + PIECE, HD), bf16),
            pltpu.VMEM((cache_rows + PIECE, HD), bf16),
            pltpu.VMEM((2 * kv_heads, SEQ_BLOCK, cache_len, 2, HD), bf16),
            pltpu.VMEM((2 * cache_rows, HD), jnp.float32),
            pltpu.VMEM((unit, exponents.shape[1]), jnp.int32),
            pltpu.VMEM((unit, 128), jnp.float32),
            dma((4,)),
            dma((2, kv_heads)),
            dma((2,)),
            dma((batches,)),
            dma((units - batches, 2)),
            dma((units - batches, 2)),
            dma((units - batches, 2)),
            dma((units - batches, 2)),
        ],
        compiler_params=pltpu.CompilerParams(
            collective_id=0, has_side_effects=True, vmem_limit_bytes=67043328
        ),
    )(
        tokens,
        norm_gain.reshape(1, depth),
        query_weight,
        key_weight,
        value_weight,
        out_weight,
        past_cache,
        exponents,
        cosine,
        sine_part,
        bias,
    )


def solution(mesh):
    return jax.shard_map(
        on_device,
        mesh=mesh,
        in_specs=(
            P(("dp", "tensor"), None),
            P(),
            P(None, "tensor"),
            P(None, "tensor"),
            P(None, "tensor"),
            P("tensor", None),
            P("dp", None, None, "tensor"),
            P("dp", None),
        ),
        out_specs=P(("dp", "tensor"), None),
        check_vma=False,
    )
```

```python
import functools

import jax
import jax.numpy as jnp
import numpy as np
from jax import lax
from jax.experimental import pallas as pl
from jax.experimental.pallas import tpu as pltpu
from jax.sharding import PartitionSpec as P

HD = 128
NEW = 10
SEQ_BLOCK = 8
PIECE = SEQ_BLOCK * NEW
WIDTH = 512
SPLIT = 2
LAST = ((0, 48), (48, 32))

epsilon = 1e-05
theta_base = 500000.0
MESH = pl.DeviceIdType.MESH


def rotary_tables(cache_len):
    half_dim = HD // 2
    positions = np.arange(PIECE) % NEW + cache_len
    frequency = theta_base ** (-(np.arange(half_dim) * 2.0) / HD)
    angles = positions[:, None] * frequency[None, :]
    cosine = np.cos(angles)
    sine_part = np.sin(angles)
    return (
        np.concatenate([cosine, cosine], 1).astype(np.float32),
        np.concatenate([-sine_part, sine_part], 1).astype(np.float32),
    )


def mask_table(cache_len):
    row = np.arange(PIECE)[:, None]
    cached = np.arange(SEQ_BLOCK * cache_len)[None, :]
    fresh = np.arange(PIECE)[None, :]
    in_cache = row // NEW == cached // cache_len
    in_new = (row // NEW == fresh // NEW) & (row % NEW >= fresh % NEW)
    return np.where(np.concatenate([in_cache, in_new], 1), 0.0, -1e30).astype(np.float32)


def ring_index(place, ranks):
    half = ranks // 2
    return jnp.where(place < half, place, half + ranks - 1 - place)


def layer_kernel(
    ranks,
    batches,
    tokens_ref,
    gain_ref,
    wq_ref,
    wk_ref,
    wv_ref,
    wo_ref,
    cache_ref,
    expo_ref,
    cos_ref,
    sin_ref,
    bias_ref,
    out_ref,
    slots,
    sums,
    wq,
    wk,
    wv,
    wo,
    heads,
    key_new,
    value_new,
    keys,
    values,
    raw,
    wide,
    gain,
    powers,
    scale,
    local_sem,
    raw_sem,
    token_sem,
    out_sem,
    gather_send,
    gather_recv,
    reduce_send,
    reduce_recv,
    last_send,
    last_recv,
):
    unit = 2 * PIECE
    units = ranks * batches
    own_rows = unit * batches
    depth = slots.shape[2]
    q_cols = heads.shape[1]
    kv_heads = key_new.shape[1] // HD
    group = q_cols // (kv_heads * HD)
    cache_len = cache_ref.shape[1]
    cache_rows = SEQ_BLOCK * cache_len
    groups = expo_ref.shape[0]
    group_cols = depth // groups
    inv_root = 1.0 / HD**0.5

    me = lax.axis_index("tensor")
    place = ring_index(me, ranks)
    right = ring_index(lax.rem(place + 1, ranks), ranks)
    left = ring_index(lax.rem(place + ranks - 1, ranks), ranks)

    def half(d):
        return pl.ds(d * PIECE, PIECE)

    def piece_row(k, d):
        hop, batch = k // batches, k % batches
        source = lax.rem(place + ranks - hop, ranks) if d == 0 else lax.rem(place + hop, ranks)
        return ring_index(source, ranks) * own_rows + (2 * batch + d) * PIECE

    weight_copies = [
        pltpu.make_async_copy(src, dst, local_sem.at[i])
        for i, (src, dst) in enumerate(
            ((wq_ref, wq), (wk_ref, wk), (wv_ref, wv), (wo_ref, wo))
        )
    ]

    def first_copy(b, d):
        return pltpu.make_async_copy(
            tokens_ref.at[pl.ds(b * unit + d * PIECE, PIECE), :],
            slots.at[batches + b, half(d), :],
            token_sem.at[b, d],
        )

    def token_copy(b):
        return pltpu.make_async_copy(
            tokens_ref.at[pl.ds(b * unit, unit), :], slots.at[units + b], token_sem.at[b, 0]
        )

    def out_copy(b, d, part):
        first, size = LAST[part]
        return pltpu.make_async_copy(
            slots.at[units + b, pl.ds(d * PIECE + first, size), :],
            out_ref.at[pl.ds(b * unit + d * PIECE + first, size), :],
            out_sem.at[b, d, part],
        )

    def last_copy(k, d, part):
        first, size = LAST[part]
        rows = pl.ds(d * PIECE + first, size)
        return pltpu.make_async_remote_copy(
            src_ref=slots.at[k, rows, :],
            dst_ref=sums.at[k - batches, rows, :],
            send_sem=last_send.at[k - units + batches, d, part],
            recv_sem=last_recv.at[k - units + batches, d, part],
            device_id={"tensor": right if d == 0 else left},
            device_id_type=MESH,
        )

    def raw_copy(k, d, kv):
        first = piece_row(k, d) // NEW
        return pltpu.make_async_copy(
            cache_ref.at[pl.ds(first, SEQ_BLOCK), :, :, pl.ds(kv * HD, HD)],
            raw.at[d * kv_heads + kv],
            raw_sem.at[d, kv],
        )

    def power_rows(k, d):
        return powers[pl.ds(pl.multiple_of(piece_row(k, d), PIECE), PIECE), :].astype(jnp.float32)

    def gather_copy(k, d):
        return pltpu.make_async_remote_copy(
            src_ref=slots.at[k + batches, half(d), :],
            dst_ref=slots.at[k + 2 * batches, half(d), :],
            send_sem=gather_send.at[k, d],
            recv_sem=gather_recv.at[k, d],
            device_id={"tensor": right if d == 0 else left},
            device_id_type=MESH,
        )

    def reduce_copy(k, d):
        return pltpu.make_async_remote_copy(
            src_ref=slots.at[k, half(d), :],
            dst_ref=sums.at[k - batches, half(d), :],
            send_sem=reduce_send.at[k - batches, d],
            recv_sem=reduce_recv.at[k - batches, d],
            device_id={"tensor": right if d == 0 else left},
            device_id_type=MESH,
        )

    for d in range(2):
        first_copy(0, d).start()

    barrier = pltpu.get_barrier_semaphore()
    for neighbour in (left, right):
        pl.semaphore_signal(
            barrier, inc=1, device_id={"tensor": neighbour}, device_id_type=MESH
        )

    def norm(slot, d):
        def step(i, carry):
            rows = pl.ds(pl.multiple_of(d * PIECE + i * 16, 16), 16)
            floats = slots[slot, rows, :].astype(jnp.float32)
            normed = floats * lax.rsqrt(jnp.mean(floats * floats, axis=-1, keepdims=True) + epsilon)
            slots[slot, rows, :] = (normed * gain[...]).astype(jnp.bfloat16)
            return carry

        lax.fori_loop(0, PIECE // 16, step, 0)

    gain[...] = gain_ref[...].astype(jnp.float32).reshape(1, depth)
    for d in range(2):
        first_copy(0, d).wait()
        if d == 0:
            for b in range(1, batches):
                for e in range(2):
                    first_copy(b, e).start()
            for copy in weight_copies:
                copy.start()
        norm(batches, d)
        if d == 0:
            pl.semaphore_wait(barrier, 2)
        gather_copy(0, d).start()
    for d in range(2):
        for kv in range(kv_heads):
            raw_copy(0, d, kv).start()
    for b in range(1, batches):
        for d in range(2):
            first_copy(b, d).wait()
            norm(batches + b, d)
            gather_copy(b, d).start()
    token_total = powers.shape[0]
    for first in range(0, token_total, 128):
        size = min(128, token_total - first)
        block = expo_ref[:, first : first + size].astype(jnp.float32)
        block = jnp.concatenate([block, jnp.zeros((128 - groups, size), jnp.float32)], 0)
        powers[first : first + size, :] = block.T.astype(jnp.bfloat16)

    def turn(block):
        cosine = cos_ref[...]
        sine_part = sin_ref[...]
        parts = []
        for d in range(2):
            turned = []
            for h in range(block.shape[1] // HD):
                head = block[d * PIECE : (d + 1) * PIECE, h * HD : (h + 1) * HD]
                turned.append(head * cosine + pltpu.roll(head, HD // 2, 1) * sine_part)
            parts.append(jnp.concatenate(turned, 1) if len(turned) > 1 else turned[0])
        return jnp.concatenate(parts, 0)

    def project(k):
        slot = k + batches
        width = min(WIDTH, q_cols)

        def tile(j, carry):
            cols = pl.ds(pl.multiple_of(j * width, width), width)
            query = jnp.dot(slots[slot], wq[:, cols], preferred_element_type=jnp.float32)
            heads[:, cols] = turn(query).astype(jnp.bfloat16)
            return carry

        lax.fori_loop(0, q_cols // width, tile, 0)
        key = jnp.dot(slots[slot], wk[...], preferred_element_type=jnp.float32)
        key_new[...] = turn(key).astype(jnp.bfloat16)
        value = jnp.dot(slots[slot], wv[...], preferred_element_type=jnp.float32)
        value_new[...] = value.astype(jnp.bfloat16)

    def attend(k, d):
        rows = half(d)
        bias = bias_ref[...]
        for kv in range(kv_heads):
            raw_copy(k, d, kv).wait()
            span = slice(kv * HD, (kv + 1) * HD)
            pairs = raw.at[d * kv_heads + kv].reshape(2 * cache_rows, HD)
            some = cache_rows // 2
            for part in range(2):
                wide[...] = pairs[part * cache_rows : (part + 1) * cache_rows].astype(jnp.float32)
                span_rows = slice(part * some, (part + 1) * some)
                keys[span_rows] = wide[pl.ds(0, some, 2), :].astype(jnp.bfloat16)
                values[span_rows] = wide[pl.ds(1, some, 2), :].astype(jnp.bfloat16)
            keys[cache_rows:] = key_new[rows, span]
            values[cache_rows:] = value_new[rows, span]

            @pl.when(k + 1 < units)
            def _():
                raw_copy(k + 1, d, kv).start()

            base = kv * group * HD
            count = max(group // SPLIT, 1)
            for first in range(0, group, count):
                start = base + first * HD
                query = jnp.concatenate(
                    [heads[rows, start + g * HD : start + (g + 1) * HD] for g in range(count)], 0
                )
                scores = lax.dot_general(
                    query, keys[...], (((1,), (1,)), ((), ())), preferred_element_type=jnp.float32
                )
                weights = []
                for g in range(count):
                    part = scores[g * PIECE : (g + 1) * PIECE] * inv_root + bias
                    probs = jnp.exp(part - jnp.max(part, axis=-1, keepdims=True))
                    total = 1.0 / jnp.sum(probs, axis=-1, keepdims=True)
                    weights.append((probs * total).astype(jnp.bfloat16))
                combined = jnp.dot(
                    jnp.concatenate(weights, 0), values[...], preferred_element_type=jnp.float32
                ).astype(jnp.bfloat16)
                for g in range(count):
                    heads[rows, start + g * HD : start + (g + 1) * HD] = combined[
                        g * PIECE : (g + 1) * PIECE
                    ]

    def project_out(k):
        for d in range(2):
            scale[half(d), :] = jnp.exp2(-power_rows(k, d))

        per_tile = WIDTH // group_cols

        def tile(j, carry):
            cols = pl.ds(pl.multiple_of(j * WIDTH, WIDTH), WIDTH)
            partial_value = jnp.dot(heads[...], wo[:, cols], preferred_element_type=jnp.float32)
            shrink = scale[...]
            parts = []
            for i in range(per_tile):
                part = partial_value[:, i * group_cols : (i + 1) * group_cols]
                parts.append(jnp.clip(part * shrink[:, i : i + 1], -127.0, 127.0))
            slots[k, :, cols] = jnp.concatenate(parts, 1).astype(jnp.bfloat16)
            scale[...] = pltpu.roll(shrink, shrink.shape[1] - per_tile, 1)
            return carry

        lax.fori_loop(0, depth // WIDTH, tile, 0)

    def add_sums(k):
        def step(i, carry):
            rows = pl.ds(pl.multiple_of(i * 16, 16), 16)
            slots[k, rows, :] = (
                slots[k, rows, :].astype(jnp.float32)
                + sums[k - 2 * batches, rows, :].astype(jnp.float32)
            ).astype(jnp.bfloat16)
            return carry

        lax.fori_loop(0, unit // 16, step, 0)

    def body(k, carry):
        @pl.when(k >= units - batches)
        def _():
            for d in range(2):
                gather_copy(k - batches, d).wait_recv()

        @pl.when(k == 0)
        def _():
            for copy in weight_copies[:3]:
                copy.wait()

        project(k)
        for d in range(2):
            attend(k, d)

        @pl.when(k + 2 * batches < units)
        def _():
            for d in range(2):
                gather_copy(k, d).wait_recv()
                gather_copy(k + batches, d).start()

        @pl.when(k == 0)
        def _():
            weight_copies[3].wait()

        @pl.when(k >= batches)
        def _():
            for d in range(2):
                gather_copy(k - batches, d).wait_send()

        project_out(k)

        @pl.when(k >= 2 * batches)
        def _():
            for d in range(2):
                reduce_copy(k - batches, d).wait_recv()
            add_sums(k)

        @pl.when((k >= batches) & (k < units - batches))
        def _():
            for d in range(2):
                reduce_copy(k, d).start()

        @pl.when(k >= units - batches)
        def _():
            for part in range(len(LAST)):
                for d in range(2):
                    last_copy(k, d, part).start()

        return carry

    lax.fori_loop(0, units, body, 0)

    for b in range(batches):
        token_copy(b).start()
    for b in range(batches):
        token_copy(b).wait()
        for d in range(2):
            scale[half(d), :] = jnp.exp2(power_rows(b, d))
        for part, (first, size) in enumerate(LAST):
            for d in range(2):
                last_copy(units - batches + b, d, part).wait_recv()

                def step(i, carry):
                    rows = pl.ds(pl.multiple_of(d * PIECE + first + i * 16, 16), 16)
                    for g in range(groups):
                        cols = slice(g * group_cols, (g + 1) * group_cols)
                        total = slots[b, rows, cols].astype(jnp.float32) + sums[
                            units - 2 * batches + b, rows, cols
                        ].astype(jnp.float32)
                        term = total * scale[rows, g : g + 1]
                        slots[units + b, rows, cols] = (
                            slots[units + b, rows, cols].astype(jnp.float32) + term
                        ).astype(jnp.bfloat16)
                    return carry

                lax.fori_loop(0, size // 16, step, 0)
                out_copy(b, d, part).start()

    def drain(k, carry):
        for d in range(2):
            reduce_copy(k, d).wait_send()
        return carry

    lax.fori_loop(batches, units - batches, drain, 0)
    for b in range(batches):
        for part in range(len(LAST)):
            for d in range(2):
                last_copy(units - batches + b, d, part).wait_send()
                out_copy(b, d, part).wait()


def on_device(
    tokens, norm_gain, query_weight, key_weight, value_weight, out_weight, past_cache, exponents
):
    own_rows, depth = tokens.shape
    ranks = lax.axis_size("tensor")
    unit = 2 * PIECE
    batches = own_rows // unit
    units = ranks * batches
    q_cols = query_weight.shape[1]
    k_cols = key_weight.shape[1]
    kv_heads = k_cols // HD
    cache_len = past_cache.shape[1]
    cache_rows = SEQ_BLOCK * cache_len
    cosine, sine_part = rotary_tables(cache_len)
    bias = mask_table(cache_len)
    any_spec = pl.BlockSpec(memory_space=pl.ANY)
    vmem_spec = pl.BlockSpec(memory_space=pltpu.VMEM)
    bf16 = jnp.bfloat16
    dma = pltpu.SemaphoreType.DMA
    return pl.pallas_call(
        functools.partial(layer_kernel, ranks, batches),
        in_specs=[any_spec, vmem_spec] + [any_spec] * 5 + [vmem_spec] * 4,
        out_specs=any_spec,
        out_shape=jax.ShapeDtypeStruct(tokens.shape, bf16),
        scratch_shapes=[
            pltpu.VMEM((units + batches, unit, depth), bf16),
            pltpu.VMEM((units - batches, unit, depth), bf16),
            pltpu.VMEM((depth, q_cols), bf16),
            pltpu.VMEM((depth, k_cols), bf16),
            pltpu.VMEM((depth, k_cols), bf16),
            pltpu.VMEM((q_cols, depth), bf16),
            pltpu.VMEM((unit, q_cols), bf16),
            pltpu.VMEM((unit, k_cols), bf16),
            pltpu.VMEM((unit, k_cols), bf16),
            pltpu.VMEM((cache_rows + PIECE, HD), bf16),
            pltpu.VMEM((cache_rows + PIECE, HD), bf16),
            pltpu.VMEM((2 * kv_heads, SEQ_BLOCK, cache_len, 2, HD), bf16),
            pltpu.VMEM((cache_rows, HD), jnp.float32),
            pltpu.VMEM((1, depth), jnp.float32),
            pltpu.VMEM((exponents.shape[0], 128), bf16),
            pltpu.VMEM((unit, 128), jnp.float32),
            dma((4,)),
            dma((2, kv_heads)),
            dma((batches, 2)),
            dma((batches, 2, len(LAST))),
            dma((units - batches, 2)),
            dma((units - batches, 2)),
            dma((units - batches, 2)),
            dma((units - batches, 2)),
            dma((batches, 2, len(LAST))),
            dma((batches, 2, len(LAST))),
        ],
        compiler_params=pltpu.CompilerParams(
            collective_id=0, has_side_effects=True, vmem_limit_bytes=67043328
        ),
    )(
        tokens,
        norm_gain,
        query_weight,
        key_weight,
        value_weight,
        out_weight,
        past_cache,
        exponents.T,
        cosine,
        sine_part,
        bias,
    )


def solution(mesh):
    return jax.shard_map(
        on_device,
        mesh=mesh,
        in_specs=(
            P(("dp", "tensor"), None),
            P(),
            P(None, "tensor"),
            P(None, "tensor"),
            P(None, "tensor"),
            P("tensor", None),
            P("dp", None, None, "tensor"),
            P("dp", None),
        ),
        out_specs=P(("dp", "tensor"), None),
        check_vma=False,
    )
```

```python
import functools

import jax
import jax.numpy as jnp
import numpy as np
from jax import lax
from jax.experimental import pallas as pl
from jax.experimental.pallas import tpu as pltpu
from jax.sharding import PartitionSpec as P

HD = 128
NEW = 10
SEQ_BLOCK = 8
PIECE = SEQ_BLOCK * NEW
WIDTH = 512
SPLIT = 2
FIRST = ((0, 16), (16, 32), (48, 32))
LAST = ((0, 48), (48, 16), (64, 16))
COPY_ROWS = 32

epsilon = 1e-05
theta_base = 500000.0
MESH = pl.DeviceIdType.MESH


def rotary_tables(cache_len):
    half_dim = HD // 2
    positions = np.arange(PIECE) % NEW + cache_len
    frequency = theta_base ** (-(np.arange(half_dim) * 2.0) / HD)
    angles = positions[:, None] * frequency[None, :]
    cosine = np.cos(angles)
    sine_part = np.sin(angles)
    return (
        np.concatenate([cosine, cosine], 1).astype(np.float32),
        np.concatenate([-sine_part, sine_part], 1).astype(np.float32),
    )


def mask_table(cache_len):
    row = np.arange(PIECE)[:, None]
    cached = np.arange(SEQ_BLOCK * cache_len)[None, :]
    fresh = np.arange(PIECE)[None, :]
    in_cache = row // NEW == cached // cache_len
    in_new = (row // NEW == fresh // NEW) & (row % NEW >= fresh % NEW)
    return np.where(np.concatenate([in_cache, in_new], 1), 0.0, -1e30).astype(np.float32)


def ring_index(place, ranks):
    half = ranks // 2
    return jnp.where(place < half, place, half + ranks - 1 - place)


def layer_kernel(
    ranks,
    batches,
    tokens_ref,
    gain_in,
    wq_ref,
    wk_ref,
    wv_ref,
    wo_ref,
    cache_ref,
    expo_in,
    cos_in,
    sin_in,
    bias_in,
    out_ref,
    slots,
    sums,
    wq,
    wk,
    wv,
    wo,
    heads,
    key_new,
    value_new,
    keys,
    values,
    raw,
    wide,
    gain_ref,
    expo_ref,
    cos_ref,
    sin_ref,
    bias_ref,
    gain,
    powers,
    scale,
    local_sem,
    small_sem,
    raw_sem,
    token_sem,
    out_sem,
    gather_send,
    gather_recv,
    reduce_send,
    reduce_recv,
    last_send,
    last_recv,
):
    unit = 2 * PIECE
    units = ranks * batches
    own_rows = unit * batches
    depth = slots.shape[2]
    q_cols = heads.shape[1]
    kv_heads = key_new.shape[1] // HD
    group = q_cols // (kv_heads * HD)
    cache_len = cache_ref.shape[1]
    cache_rows = SEQ_BLOCK * cache_len
    groups = expo_in.shape[0]
    group_cols = depth // groups
    inv_root = 1.0 / HD**0.5

    me = lax.axis_index("tensor")
    place = ring_index(me, ranks)
    right = ring_index(lax.rem(place + 1, ranks), ranks)
    left = ring_index(lax.rem(place + ranks - 1, ranks), ranks)

    def half(d):
        return pl.ds(d * PIECE, PIECE)

    def piece_row(k, d):
        hop, batch = k // batches, k % batches
        source = lax.rem(place + ranks - hop, ranks) if d == 0 else lax.rem(place + hop, ranks)
        return ring_index(source, ranks) * own_rows + (2 * batch + d) * PIECE

    weight_copies = [
        pltpu.make_async_copy(src, dst, local_sem.at[i])
        for i, (src, dst) in enumerate(
            ((wq_ref, wq), (wk_ref, wk), (wv_ref, wv), (wo_ref, wo))
        )
    ]

    small_copies = [
        pltpu.make_async_copy(src, dst, small_sem.at[i])
        for i, (src, dst) in enumerate(
            (
                (gain_in, gain_ref),
                (expo_in, expo_ref),
                (cos_in, cos_ref),
                (sin_in, sin_ref),
                (bias_in, bias_ref),
            )
        )
    ]

    def first_copy(b, d, part, rows):
        first, size = rows
        return pltpu.make_async_copy(
            tokens_ref.at[pl.ds(b * unit + d * PIECE + first, size), :],
            slots.at[batches + b, pl.ds(d * PIECE + first, size), :],
            token_sem.at[b, d, part],
        )

    def token_copy(b):
        return pltpu.make_async_copy(
            tokens_ref.at[pl.ds(b * unit, unit), :], slots.at[units + b], token_sem.at[b, 0, 0]
        )

    def out_copy(b, d, part):
        first, size = LAST[part]
        return pltpu.make_async_copy(
            slots.at[units + b, pl.ds(d * PIECE + first, size), :],
            out_ref.at[pl.ds(b * unit + d * PIECE + first, size), :],
            out_sem.at[b, d, part],
        )

    def last_copy(k, d, part):
        first, size = LAST[part]
        rows = pl.ds(d * PIECE + first, size)
        return pltpu.make_async_remote_copy(
            src_ref=slots.at[k, rows, :],
            dst_ref=sums.at[k - batches, rows, :],
            send_sem=last_send.at[k - units + batches, d, part],
            recv_sem=last_recv.at[k - units + batches, d, part],
            device_id={"tensor": right if d == 0 else left},
            device_id_type=MESH,
        )

    def raw_copy(k, d, kv):
        first = piece_row(k, d) // NEW
        return pltpu.make_async_copy(
            cache_ref.at[pl.ds(first, SEQ_BLOCK), :, :, pl.ds(kv * HD, HD)],
            raw.at[d * kv_heads + kv],
            raw_sem.at[d, kv],
        )

    def power_rows(k, d):
        return powers[pl.ds(pl.multiple_of(piece_row(k, d), PIECE), PIECE), :].astype(jnp.float32)

    def gather_copy(k, d, rows=(0, PIECE)):
        span = pl.ds(d * PIECE + rows[0], rows[1])
        return pltpu.make_async_remote_copy(
            src_ref=slots.at[k + batches, span, :],
            dst_ref=slots.at[k + 2 * batches, span, :],
            send_sem=gather_send.at[k, d],
            recv_sem=gather_recv.at[k, d],
            device_id={"tensor": right if d == 0 else left},
            device_id_type=MESH,
        )

    def reduce_copy(k, d):
        return pltpu.make_async_remote_copy(
            src_ref=slots.at[k, half(d), :],
            dst_ref=sums.at[k - batches, half(d), :],
            send_sem=reduce_send.at[k - batches, d],
            recv_sem=reduce_recv.at[k - batches, d],
            device_id={"tensor": right if d == 0 else left},
            device_id_type=MESH,
        )

    barrier = pltpu.get_barrier_semaphore()
    for neighbour in (left, right):
        pl.semaphore_signal(
            barrier, inc=1, device_id={"tensor": neighbour}, device_id_type=MESH
        )

    small_copies[0].start()
    for part, rows in enumerate(FIRST):
        for d in range(2):
            first_copy(0, d, part, rows).start()

    def norm(slot, d, first, size):
        def step(i, carry):
            rows = pl.ds(pl.multiple_of(d * PIECE + first + i * 16, 16), 16)
            floats = slots[slot, rows, :].astype(jnp.float32)
            normed = floats * lax.rsqrt(jnp.mean(floats * floats, axis=-1, keepdims=True) + epsilon)
            slots[slot, rows, :] = (normed * gain[...]).astype(jnp.bfloat16)
            return carry

        lax.fori_loop(0, size // 16, step, 0)

    small_copies[0].wait()
    gain[...] = gain_ref[...].astype(jnp.float32).reshape(1, depth)
    whole = (0, PIECE)
    for part, rows in enumerate(FIRST):
        for d in range(2):
            first_copy(0, d, part, rows).wait()
            norm(batches, d, *rows)
            if part == 0 and d == 0:
                pl.semaphore_wait(barrier, 2)
            gather_copy(0, d, rows).start()
        if part == 0:
            for b in range(1, batches):
                for d in range(2):
                    first_copy(b, d, 0, whole).start()
            for copy in weight_copies + small_copies[1:]:
                copy.start()
            for d in range(2):
                for kv in range(kv_heads):
                    raw_copy(0, d, kv).start()
    for b in range(1, batches):
        for d in range(2):
            first_copy(b, d, 0, whole).wait()
            norm(batches + b, d, *whole)
            gather_copy(b, d).start()
    for copy in small_copies[1:]:
        copy.wait()
    token_total = powers.shape[0]
    for first in range(0, token_total, 128):
        size = min(128, token_total - first)
        block = expo_ref[:, first : first + size].astype(jnp.float32)
        block = jnp.concatenate([block, jnp.zeros((128 - groups, size), jnp.float32)], 0)
        powers[first : first + size, :] = block.T.astype(jnp.bfloat16)

    def turn(block):
        cosine = cos_ref[...]
        sine_part = sin_ref[...]
        parts = []
        for d in range(2):
            turned = []
            for h in range(block.shape[1] // HD):
                head = block[d * PIECE : (d + 1) * PIECE, h * HD : (h + 1) * HD]
                turned.append(head * cosine + pltpu.roll(head, HD // 2, 1) * sine_part)
            parts.append(jnp.concatenate(turned, 1) if len(turned) > 1 else turned[0])
        return jnp.concatenate(parts, 0)

    def project(k):
        slot = k + batches
        width = min(WIDTH, q_cols)

        def tile(j, carry):
            cols = pl.ds(pl.multiple_of(j * width, width), width)
            query = jnp.dot(slots[slot], wq[:, cols], preferred_element_type=jnp.float32)
            heads[:, cols] = turn(query).astype(jnp.bfloat16)
            return carry

        lax.fori_loop(0, q_cols // width, tile, 0)
        key = jnp.dot(slots[slot], wk[...], preferred_element_type=jnp.float32)
        key_new[...] = turn(key).astype(jnp.bfloat16)
        value = jnp.dot(slots[slot], wv[...], preferred_element_type=jnp.float32)
        value_new[...] = value.astype(jnp.bfloat16)

    def attend(k, d):
        rows = half(d)
        bias = bias_ref[...]
        for kv in range(kv_heads):
            raw_copy(k, d, kv).wait()
            span = slice(kv * HD, (kv + 1) * HD)
            pairs = raw.at[d * kv_heads + kv].reshape(2 * cache_rows, HD)
            some = cache_rows // 2
            for part in range(2):
                wide[...] = pairs[part * cache_rows : (part + 1) * cache_rows].astype(jnp.float32)
                span_rows = slice(part * some, (part + 1) * some)
                keys[span_rows] = wide[pl.ds(0, some, 2), :].astype(jnp.bfloat16)
                values[span_rows] = wide[pl.ds(1, some, 2), :].astype(jnp.bfloat16)
            keys[cache_rows:] = key_new[rows, span]
            values[cache_rows:] = value_new[rows, span]

            @pl.when(k + 1 < units)
            def _():
                raw_copy(k + 1, d, kv).start()

            base = kv * group * HD
            count = max(group // SPLIT, 1)
            for first in range(0, group, count):
                start = base + first * HD
                query = jnp.concatenate(
                    [heads[rows, start + g * HD : start + (g + 1) * HD] for g in range(count)], 0
                )
                scores = lax.dot_general(
                    query, keys[...], (((1,), (1,)), ((), ())), preferred_element_type=jnp.float32
                )
                weights = []
                for g in range(count):
                    part = scores[g * PIECE : (g + 1) * PIECE] * inv_root + bias
                    probs = jnp.exp(part - jnp.max(part, axis=-1, keepdims=True))
                    total = 1.0 / jnp.sum(probs, axis=-1, keepdims=True)
                    weights.append((probs * total).astype(jnp.bfloat16))
                combined = jnp.dot(
                    jnp.concatenate(weights, 0), values[...], preferred_element_type=jnp.float32
                ).astype(jnp.bfloat16)
                for g in range(count):
                    heads[rows, start + g * HD : start + (g + 1) * HD] = combined[
                        g * PIECE : (g + 1) * PIECE
                    ]

    def project_out(k):
        for d in range(2):
            scale[half(d), :] = jnp.exp2(-power_rows(k, d))

        per_tile = WIDTH // group_cols

        def tile(j, carry):
            cols = pl.ds(pl.multiple_of(j * WIDTH, WIDTH), WIDTH)
            partial_value = jnp.dot(heads[...], wo[:, cols], preferred_element_type=jnp.float32)
            shrink = scale[...]
            parts = []
            for i in range(per_tile):
                part = partial_value[:, i * group_cols : (i + 1) * group_cols]
                parts.append(jnp.clip(part * shrink[:, i : i + 1], -127.0, 127.0))
            slots[k, :, cols] = jnp.concatenate(parts, 1).astype(jnp.bfloat16)
            scale[...] = pltpu.roll(shrink, shrink.shape[1] - per_tile, 1)
            return carry

        lax.fori_loop(0, depth // WIDTH, tile, 0)

    def add_sums(k):
        def step(i, carry):
            rows = pl.ds(pl.multiple_of(i * 16, 16), 16)
            slots[k, rows, :] = (
                slots[k, rows, :].astype(jnp.float32)
                + sums[k - 2 * batches, rows, :].astype(jnp.float32)
            ).astype(jnp.bfloat16)
            return carry

        lax.fori_loop(0, unit // 16, step, 0)

    def body(k, carry):
        @pl.when(k >= units - batches)
        def _():
            for d in range(2):
                gather_copy(k - batches, d).wait_recv()

        @pl.when(k == 0)
        def _():
            for copy in weight_copies[:3]:
                copy.wait()

        project(k)
        for d in range(2):
            attend(k, d)

        @pl.when(k + 2 * batches < units)
        def _():
            for d in range(2):
                gather_copy(k, d).wait_recv()
                gather_copy(k + batches, d).start()

        @pl.when(k == 0)
        def _():
            weight_copies[3].wait()

        @pl.when(k >= batches)
        def _():
            for d in range(2):
                gather_copy(k - batches, d).wait_send()

        project_out(k)

        @pl.when(k >= 2 * batches)
        def _():
            for d in range(2):
                reduce_copy(k - batches, d).wait_recv()
            add_sums(k)

        @pl.when((k >= batches) & (k < units - batches))
        def _():
            for d in range(2):
                reduce_copy(k, d).start()

        @pl.when(k >= units - batches)
        def _():
            for part in range(len(LAST)):
                for d in range(2):
                    last_copy(k, d, part).start()

        return carry

    lax.fori_loop(0, units, body, 0)

    for b in range(batches):
        token_copy(b).start()
    for b in range(batches):
        token_copy(b).wait()
        for d in range(2):
            scale[half(d), :] = jnp.exp2(power_rows(b, d))
        for part, (first, size) in enumerate(LAST):
            for d in range(2):
                last_copy(units - batches + b, d, part).wait_recv()

                def step(i, carry):
                    rows = pl.ds(pl.multiple_of(d * PIECE + first + i * 16, 16), 16)
                    for g in range(groups):
                        cols = slice(g * group_cols, (g + 1) * group_cols)
                        total = slots[b, rows, cols].astype(jnp.float32) + sums[
                            units - 2 * batches + b, rows, cols
                        ].astype(jnp.float32)
                        term = total * scale[rows, g : g + 1]
                        slots[units + b, rows, cols] = (
                            slots[units + b, rows, cols].astype(jnp.float32) + term
                        ).astype(jnp.bfloat16)
                    return carry

                lax.fori_loop(0, size // 16, step, 0)
                out_copy(b, d, part).start()

    def drain(k, carry):
        for d in range(2):
            reduce_copy(k, d).wait_send()
        return carry

    lax.fori_loop(batches, units - batches, drain, 0)
    for b in range(batches):
        for part in range(len(LAST)):
            for d in range(2):
                last_copy(units - batches + b, d, part).wait_send()
                out_copy(b, d, part).wait()


def copy_kernel(src_ref, out_ref, held, in_sem, out_sem):
    count = src_ref.shape[0] // COPY_ROWS

    def move(src, dst, sem, i):
        rows = pl.ds(i * COPY_ROWS, COPY_ROWS)
        return pltpu.make_async_copy(src.at[rows, :], dst.at[rows, :], sem.at[i])

    for i in range(count):
        move(src_ref, held, in_sem, i).start()
    for i in range(count):
        move(src_ref, held, in_sem, i).wait()
        move(held, out_ref, out_sem, i).start()
    for i in range(count):
        move(held, out_ref, out_sem, i).wait()


def copy_out(mixed):
    count = mixed.shape[0] // COPY_ROWS
    any_spec = pl.BlockSpec(memory_space=pl.ANY)
    return pl.pallas_call(
        copy_kernel,
        in_specs=[any_spec],
        out_specs=any_spec,
        out_shape=jax.ShapeDtypeStruct(mixed.shape, mixed.dtype),
        scratch_shapes=[
            pltpu.VMEM(mixed.shape, mixed.dtype),
            pltpu.SemaphoreType.DMA((count,)),
            pltpu.SemaphoreType.DMA((count,)),
        ],
        compiler_params=pltpu.CompilerParams(vmem_limit_bytes=56 * 1024 * 1024),
    )(mixed)


def on_device(
    tokens, norm_gain, query_weight, key_weight, value_weight, out_weight, past_cache, exponents
):
    own_rows, depth = tokens.shape
    ranks = lax.axis_size("tensor")
    unit = 2 * PIECE
    batches = own_rows // unit
    units = ranks * batches
    q_cols = query_weight.shape[1]
    k_cols = key_weight.shape[1]
    kv_heads = k_cols // HD
    cache_len = past_cache.shape[1]
    cache_rows = SEQ_BLOCK * cache_len
    cosine, sine_part = rotary_tables(cache_len)
    bias = mask_table(cache_len)
    any_spec = pl.BlockSpec(memory_space=pl.ANY)
    bf16 = jnp.bfloat16
    dma = pltpu.SemaphoreType.DMA
    mixed = pl.pallas_call(
        functools.partial(layer_kernel, ranks, batches),
        in_specs=[any_spec] * 11,
        out_specs=any_spec,
        out_shape=jax.ShapeDtypeStruct(tokens.shape, bf16),
        scratch_shapes=[
            pltpu.VMEM((units + batches, unit, depth), bf16),
            pltpu.VMEM((units - batches, unit, depth), bf16),
            pltpu.VMEM((depth, q_cols), bf16),
            pltpu.VMEM((depth, k_cols), bf16),
            pltpu.VMEM((depth, k_cols), bf16),
            pltpu.VMEM((q_cols, depth), bf16),
            pltpu.VMEM((unit, q_cols), bf16),
            pltpu.VMEM((unit, k_cols), bf16),
            pltpu.VMEM((unit, k_cols), bf16),
            pltpu.VMEM((cache_rows + PIECE, HD), bf16),
            pltpu.VMEM((cache_rows + PIECE, HD), bf16),
            pltpu.VMEM((2 * kv_heads, SEQ_BLOCK, cache_len, 2, HD), bf16),
            pltpu.VMEM((cache_rows, HD), jnp.float32),
            pltpu.VMEM(norm_gain.shape, bf16),
            pltpu.VMEM(exponents.shape[::-1], jnp.int32),
            pltpu.VMEM(cosine.shape, jnp.float32),
            pltpu.VMEM(sine_part.shape, jnp.float32),
            pltpu.VMEM(bias.shape, jnp.float32),
            pltpu.VMEM((1, depth), jnp.float32),
            pltpu.VMEM((exponents.shape[0], 128), bf16),
            pltpu.VMEM((unit, 128), jnp.float32),
            dma((4,)),
            dma((5,)),
            dma((2, kv_heads)),
            dma((batches, 2, len(FIRST))),
            dma((batches, 2, len(LAST))),
            dma((units - batches, 2)),
            dma((units - batches, 2)),
            dma((units - batches, 2)),
            dma((units - batches, 2)),
            dma((batches, 2, len(LAST))),
            dma((batches, 2, len(LAST))),
        ],
        compiler_params=pltpu.CompilerParams(
            collective_id=0, has_side_effects=True, vmem_limit_bytes=67043328
        ),
    )(
        tokens,
        norm_gain,
        query_weight,
        key_weight,
        value_weight,
        out_weight,
        past_cache,
        exponents.T,
        cosine,
        sine_part,
        bias,
    )
    return copy_out(mixed)


def solution(mesh):
    return jax.shard_map(
        on_device,
        mesh=mesh,
        in_specs=(
            P(("dp", "tensor"), None),
            P(),
            P(None, "tensor"),
            P(None, "tensor"),
            P(None, "tensor"),
            P("tensor", None),
            P("dp", None, None, "tensor"),
            P("dp", None),
        ),
        out_specs=P(("dp", "tensor"), None),
        check_vma=False,
    )
```

```python
import functools

import jax
import jax.numpy as jnp
import numpy as np
from jax import lax
from jax.experimental import pallas as pl
from jax.experimental.pallas import tpu as pltpu
from jax.sharding import PartitionSpec as P

HD = 128
NEW = 10
SEQ_BLOCK = 8
PIECE = SEQ_BLOCK * NEW
WIDTH = 512
SPLIT = 2
FIRST = ((0, 16), (16, 32), (48, 32))
LAST = ((0, 48), (48, 16), (64, 16))
COPY_ROWS = 32

epsilon = 1e-05
theta_base = 500000.0
MESH = pl.DeviceIdType.MESH


def rotary_tables(cache_len):
    half_dim = HD // 2
    positions = np.arange(PIECE) % NEW + cache_len
    frequency = theta_base ** (-(np.arange(half_dim) * 2.0) / HD)
    angles = positions[:, None] * frequency[None, :]
    cosine = np.cos(angles)
    sine_part = np.sin(angles)
    return (
        np.concatenate([cosine, cosine], 1).astype(np.float32),
        np.concatenate([-sine_part, sine_part], 1).astype(np.float32),
    )


def mask_table(cache_len):
    row = np.arange(PIECE)[:, None]
    cached = np.arange(SEQ_BLOCK * cache_len)[None, :]
    fresh = np.arange(PIECE)[None, :]
    in_cache = row // NEW == cached // cache_len
    in_new = (row // NEW == fresh // NEW) & (row % NEW >= fresh % NEW)
    return np.where(np.concatenate([in_cache, in_new], 1), 0.0, -1e30).astype(np.float32)


def ring_index(place, ranks):
    half = ranks // 2
    return jnp.where(place < half, place, half + ranks - 1 - place)


def layer_kernel(
    ranks,
    batches,
    tokens_ref,
    gain_in,
    wq_ref,
    wk_ref,
    wv_ref,
    wo_ref,
    cache_ref,
    expo_in,
    cos_in,
    sin_in,
    bias_in,
    out_ref,
    tail_own,
    tail_sum,
    tail_scale,
    slots,
    sums,
    wq,
    wk,
    wv,
    wo,
    heads,
    key_new,
    value_new,
    keys,
    values,
    raw,
    wide,
    gain_ref,
    expo_ref,
    cos_ref,
    sin_ref,
    bias_ref,
    gain,
    powers,
    scale,
    local_sem,
    small_sem,
    raw_sem,
    token_sem,
    out_sem,
    tail_sem,
    gather_send,
    gather_recv,
    reduce_send,
    reduce_recv,
    last_send,
    last_recv,
):
    unit = 2 * PIECE
    units = ranks * batches
    own_rows = unit * batches
    depth = slots.shape[2]
    q_cols = heads.shape[1]
    kv_heads = key_new.shape[1] // HD
    group = q_cols // (kv_heads * HD)
    cache_len = cache_ref.shape[1]
    cache_rows = SEQ_BLOCK * cache_len
    groups = expo_in.shape[0]
    group_cols = depth // groups
    inv_root = 1.0 / HD**0.5

    me = lax.axis_index("tensor")
    place = ring_index(me, ranks)
    right = ring_index(lax.rem(place + 1, ranks), ranks)
    left = ring_index(lax.rem(place + ranks - 1, ranks), ranks)

    def half(d):
        return pl.ds(d * PIECE, PIECE)

    def piece_row(k, d):
        hop, batch = k // batches, k % batches
        source = lax.rem(place + ranks - hop, ranks) if d == 0 else lax.rem(place + hop, ranks)
        return ring_index(source, ranks) * own_rows + (2 * batch + d) * PIECE

    weight_copies = [
        pltpu.make_async_copy(src, dst, local_sem.at[i])
        for i, (src, dst) in enumerate(
            ((wq_ref, wq), (wk_ref, wk), (wv_ref, wv), (wo_ref, wo))
        )
    ]

    small_copies = [
        pltpu.make_async_copy(src, dst, small_sem.at[i])
        for i, (src, dst) in enumerate(
            (
                (gain_in, gain_ref),
                (expo_in, expo_ref),
                (cos_in, cos_ref),
                (sin_in, sin_ref),
                (bias_in, bias_ref),
            )
        )
    ]

    def first_copy(b, d, part, rows):
        first, size = rows
        return pltpu.make_async_copy(
            tokens_ref.at[pl.ds(b * unit + d * PIECE + first, size), :],
            slots.at[batches + b, pl.ds(d * PIECE + first, size), :],
            token_sem.at[b, d, part],
        )

    def token_copy(b):
        return pltpu.make_async_copy(
            tokens_ref.at[pl.ds(b * unit, unit), :], slots.at[units + b], token_sem.at[b, 0, 0]
        )

    def out_copy(b, d, part):
        first, size = LAST[part]
        return pltpu.make_async_copy(
            slots.at[units + b, pl.ds(d * PIECE + first, size), :],
            out_ref.at[pl.ds(b * unit + d * PIECE + first, size), :],
            out_sem.at[b, d, part],
        )

    def last_copy(k, d, part, tail=False):
        first, size = LAST[part]
        rows = pl.ds(d * PIECE + first, size)
        return pltpu.make_async_remote_copy(
            src_ref=slots.at[k, rows, :],
            dst_ref=tail_sum.at[d] if tail else sums.at[k - batches, rows, :],
            send_sem=last_send.at[k - units + batches, d, part],
            recv_sem=last_recv.at[k - units + batches, d, part],
            device_id={"tensor": right if d == 0 else left},
            device_id_type=MESH,
        )

    def raw_copy(k, d, kv):
        first = piece_row(k, d) // NEW
        return pltpu.make_async_copy(
            cache_ref.at[pl.ds(first, SEQ_BLOCK), :, :, pl.ds(kv * HD, HD)],
            raw.at[d * kv_heads + kv],
            raw_sem.at[d, kv],
        )

    def power_rows(k, d):
        return powers[pl.ds(pl.multiple_of(piece_row(k, d), PIECE), PIECE), :].astype(jnp.float32)

    def gather_copy(k, d, rows=(0, PIECE)):
        span = pl.ds(d * PIECE + rows[0], rows[1])
        return pltpu.make_async_remote_copy(
            src_ref=slots.at[k + batches, span, :],
            dst_ref=slots.at[k + 2 * batches, span, :],
            send_sem=gather_send.at[k, d],
            recv_sem=gather_recv.at[k, d],
            device_id={"tensor": right if d == 0 else left},
            device_id_type=MESH,
        )

    def reduce_copy(k, d):
        return pltpu.make_async_remote_copy(
            src_ref=slots.at[k, half(d), :],
            dst_ref=sums.at[k - batches, half(d), :],
            send_sem=reduce_send.at[k - batches, d],
            recv_sem=reduce_recv.at[k - batches, d],
            device_id={"tensor": right if d == 0 else left},
            device_id_type=MESH,
        )

    barrier = pltpu.get_barrier_semaphore()
    for neighbour in (left, right):
        pl.semaphore_signal(
            barrier, inc=1, device_id={"tensor": neighbour}, device_id_type=MESH
        )

    small_copies[0].start()
    for part, rows in enumerate(FIRST):
        for d in range(2):
            first_copy(0, d, part, rows).start()

    def norm(slot, d, first, size):
        def step(i, carry):
            rows = pl.ds(pl.multiple_of(d * PIECE + first + i * 16, 16), 16)
            floats = slots[slot, rows, :].astype(jnp.float32)
            normed = floats * lax.rsqrt(jnp.mean(floats * floats, axis=-1, keepdims=True) + epsilon)
            slots[slot, rows, :] = (normed * gain[...]).astype(jnp.bfloat16)
            return carry

        lax.fori_loop(0, size // 16, step, 0)

    small_copies[0].wait()
    gain[...] = gain_ref[...].astype(jnp.float32).reshape(1, depth)
    whole = (0, PIECE)
    for part, rows in enumerate(FIRST):
        for d in range(2):
            first_copy(0, d, part, rows).wait()
            norm(batches, d, *rows)
            if part == 0 and d == 0:
                pl.semaphore_wait(barrier, 2)
            gather_copy(0, d, rows).start()
        if part == 0:
            for b in range(1, batches):
                for d in range(2):
                    first_copy(b, d, 0, whole).start()
            for copy in weight_copies + small_copies[1:]:
                copy.start()
            for d in range(2):
                for kv in range(kv_heads):
                    raw_copy(0, d, kv).start()
    for b in range(1, batches):
        for d in range(2):
            first_copy(b, d, 0, whole).wait()
            norm(batches + b, d, *whole)
            gather_copy(b, d).start()
    for copy in small_copies[1:]:
        copy.wait()
    token_total = powers.shape[0]
    for first in range(0, token_total, 128):
        size = min(128, token_total - first)
        block = expo_ref[:, first : first + size].astype(jnp.float32)
        block = jnp.concatenate([block, jnp.zeros((128 - groups, size), jnp.float32)], 0)
        powers[first : first + size, :] = block.T.astype(jnp.bfloat16)

    def turn(block):
        cosine = cos_ref[...]
        sine_part = sin_ref[...]
        parts = []
        for d in range(2):
            turned = []
            for h in range(block.shape[1] // HD):
                head = block[d * PIECE : (d + 1) * PIECE, h * HD : (h + 1) * HD]
                turned.append(head * cosine + pltpu.roll(head, HD // 2, 1) * sine_part)
            parts.append(jnp.concatenate(turned, 1) if len(turned) > 1 else turned[0])
        return jnp.concatenate(parts, 0)

    def project(k):
        slot = k + batches
        width = min(WIDTH, q_cols)

        def tile(j, carry):
            cols = pl.ds(pl.multiple_of(j * width, width), width)
            query = jnp.dot(slots[slot], wq[:, cols], preferred_element_type=jnp.float32)
            heads[:, cols] = turn(query).astype(jnp.bfloat16)
            return carry

        lax.fori_loop(0, q_cols // width, tile, 0)
        key = jnp.dot(slots[slot], wk[...], preferred_element_type=jnp.float32)
        key_new[...] = turn(key).astype(jnp.bfloat16)
        value = jnp.dot(slots[slot], wv[...], preferred_element_type=jnp.float32)
        value_new[...] = value.astype(jnp.bfloat16)

    def attend(k, d):
        rows = half(d)
        bias = bias_ref[...]
        for kv in range(kv_heads):
            raw_copy(k, d, kv).wait()
            span = slice(kv * HD, (kv + 1) * HD)
            pairs = raw.at[d * kv_heads + kv].reshape(2 * cache_rows, HD)
            some = cache_rows // 2
            for part in range(2):
                wide[...] = pairs[part * cache_rows : (part + 1) * cache_rows].astype(jnp.float32)
                span_rows = slice(part * some, (part + 1) * some)
                keys[span_rows] = wide[pl.ds(0, some, 2), :].astype(jnp.bfloat16)
                values[span_rows] = wide[pl.ds(1, some, 2), :].astype(jnp.bfloat16)
            keys[cache_rows:] = key_new[rows, span]
            values[cache_rows:] = value_new[rows, span]

            @pl.when(k + 1 < units)
            def _():
                raw_copy(k + 1, d, kv).start()

            base = kv * group * HD
            count = max(group // SPLIT, 1)
            for first in range(0, group, count):
                start = base + first * HD
                query = jnp.concatenate(
                    [heads[rows, start + g * HD : start + (g + 1) * HD] for g in range(count)], 0
                )
                scores = lax.dot_general(
                    query, keys[...], (((1,), (1,)), ((), ())), preferred_element_type=jnp.float32
                )
                weights = []
                for g in range(count):
                    part = scores[g * PIECE : (g + 1) * PIECE] * inv_root + bias
                    probs = jnp.exp(part - jnp.max(part, axis=-1, keepdims=True))
                    total = 1.0 / jnp.sum(probs, axis=-1, keepdims=True)
                    weights.append((probs * total).astype(jnp.bfloat16))
                combined = jnp.dot(
                    jnp.concatenate(weights, 0), values[...], preferred_element_type=jnp.float32
                ).astype(jnp.bfloat16)
                for g in range(count):
                    heads[rows, start + g * HD : start + (g + 1) * HD] = combined[
                        g * PIECE : (g + 1) * PIECE
                    ]

    def project_out(k):
        for d in range(2):
            scale[half(d), :] = jnp.exp2(-power_rows(k, d))

        per_tile = WIDTH // group_cols

        def tile(j, carry):
            cols = pl.ds(pl.multiple_of(j * WIDTH, WIDTH), WIDTH)
            partial_value = jnp.dot(heads[...], wo[:, cols], preferred_element_type=jnp.float32)
            shrink = scale[...]
            parts = []
            for i in range(per_tile):
                part = partial_value[:, i * group_cols : (i + 1) * group_cols]
                parts.append(jnp.clip(part * shrink[:, i : i + 1], -127.0, 127.0))
            slots[k, :, cols] = jnp.concatenate(parts, 1).astype(jnp.bfloat16)
            scale[...] = pltpu.roll(shrink, shrink.shape[1] - per_tile, 1)
            return carry

        lax.fori_loop(0, depth // WIDTH, tile, 0)

    def add_sums(k):
        def step(i, carry):
            rows = pl.ds(pl.multiple_of(i * 16, 16), 16)
            slots[k, rows, :] = (
                slots[k, rows, :].astype(jnp.float32)
                + sums[k - 2 * batches, rows, :].astype(jnp.float32)
            ).astype(jnp.bfloat16)
            return carry

        lax.fori_loop(0, unit // 16, step, 0)

    def body(k, carry):
        @pl.when(k >= units - batches)
        def _():
            for d in range(2):
                gather_copy(k - batches, d).wait_recv()

        @pl.when(k == 0)
        def _():
            for copy in weight_copies[:3]:
                copy.wait()

        project(k)
        for d in range(2):
            attend(k, d)

        @pl.when(k + 2 * batches < units)
        def _():
            for d in range(2):
                gather_copy(k, d).wait_recv()
                gather_copy(k + batches, d).start()

        @pl.when(k == 0)
        def _():
            weight_copies[3].wait()

        @pl.when(k >= batches)
        def _():
            for d in range(2):
                gather_copy(k - batches, d).wait_send()

        project_out(k)

        @pl.when(k >= 2 * batches)
        def _():
            for d in range(2):
                reduce_copy(k - batches, d).wait_recv()
            add_sums(k)

        @pl.when((k >= batches) & (k < units - batches))
        def _():
            for d in range(2):
                reduce_copy(k, d).start()

        @pl.when(k >= units - batches)
        def _():
            for part in range(len(LAST) - 1):
                for d in range(2):
                    last_copy(k, d, part).start()

        @pl.when((k >= units - batches) & (k < units - 1))
        def _():
            for d in range(2):
                last_copy(k, d, len(LAST) - 1).start()

        @pl.when(k == units - 1)
        def _():
            for d in range(2):
                last_copy(k, d, len(LAST) - 1, True).start()

        return carry

    lax.fori_loop(0, units, body, 0)

    def tail_copies(d):
        first, size = LAST[-1]
        rows = pl.ds(d * PIECE + first, size)
        return (
            pltpu.make_async_copy(
                slots.at[batches - 1, rows, :], tail_own.at[d], tail_sem.at[d, 0]
            ),
            pltpu.make_async_copy(scale.at[rows, :], tail_scale.at[d], tail_sem.at[d, 1]),
        )

    for b in range(batches):
        token_copy(b).start()
    for b in range(batches):
        token_copy(b).wait()
        for d in range(2):
            scale[half(d), :] = jnp.exp2(power_rows(b, d))
        if b == batches - 1:
            for d in range(2):
                for copy in tail_copies(d):
                    copy.start()
        for part, (first, size) in enumerate(LAST):
            for d in range(2):
                if b == batches - 1 and part == len(LAST) - 1:
                    continue
                last_copy(units - batches + b, d, part).wait_recv()

                def step(i, carry):
                    rows = pl.ds(pl.multiple_of(d * PIECE + first + i * 16, 16), 16)
                    for g in range(groups):
                        cols = slice(g * group_cols, (g + 1) * group_cols)
                        total = slots[b, rows, cols].astype(jnp.float32) + sums[
                            units - 2 * batches + b, rows, cols
                        ].astype(jnp.float32)
                        term = total * scale[rows, g : g + 1]
                        slots[units + b, rows, cols] = (
                            slots[units + b, rows, cols].astype(jnp.float32) + term
                        ).astype(jnp.bfloat16)
                    return carry

                lax.fori_loop(0, size // 16, step, 0)
                out_copy(b, d, part).start()

    def drain(k, carry):
        for d in range(2):
            reduce_copy(k, d).wait_send()
        return carry

    lax.fori_loop(batches, units - batches, drain, 0)
    for b in range(batches):
        for part in range(len(LAST)):
            for d in range(2):
                if b == batches - 1 and part == len(LAST) - 1:
                    for copy in tail_copies(d):
                        copy.wait()
                    last_copy(units - 1, d, part, True).wait_recv()
                    last_copy(units - 1, d, part, True).wait_send()
                else:
                    last_copy(units - batches + b, d, part).wait_send()
                    out_copy(b, d, part).wait()


def copy_kernel(
    groups,
    mixed_ref,
    tokens_ref,
    own_ref,
    sum_ref,
    scale_ref,
    out_ref,
    held,
    own,
    sums,
    scale,
    in_sem,
    tail_sem,
    out_sem,
):
    rows, depth = mixed_ref.shape
    first, size = LAST[-1]
    start = rows - 2 * PIECE
    tails = [start + d * PIECE + first for d in range(2)]
    edges = [0] + [edge for tail in tails for edge in (tail, tail + size)] + [rows]
    chunks = [
        (at, min(COPY_ROWS, high - at))
        for low, high in zip(edges[::2], edges[1::2])
        for at in range(low, high, COPY_ROWS)
    ]
    blocks = [(mixed_ref, at, count) for at, count in chunks]
    blocks += [(tokens_ref, at, size) for at in tails]

    def fetch(i):
        src, at, count = blocks[i]
        span = pl.ds(at, count)
        return pltpu.make_async_copy(src.at[span, :], held.at[span, :], in_sem.at[i])

    def put(i):
        _, at, count = blocks[i]
        span = pl.ds(at, count)
        return pltpu.make_async_copy(held.at[span, :], out_ref.at[span, :], out_sem.at[i])

    extras = [
        pltpu.make_async_copy(src, dst, tail_sem.at[i])
        for i, (src, dst) in enumerate(((own_ref, own), (sum_ref, sums), (scale_ref, scale)))
    ]
    order = list(range(len(chunks), len(blocks))) + list(range(len(chunks)))
    for copy in extras:
        copy.start()
    for i in order:
        fetch(i).start()
    for copy in extras:
        copy.wait()
    width = depth // groups
    for d, at in enumerate(tails):
        i = len(chunks) + d
        fetch(i).wait()
        for g in range(groups):
            cols = slice(g * width, (g + 1) * width)
            total = own[d, :, cols].astype(jnp.float32) + sums[d, :, cols].astype(jnp.float32)
            held[at : at + size, cols] = (
                held[at : at + size, cols].astype(jnp.float32) + total * scale[d, :, g : g + 1]
            ).astype(jnp.bfloat16)
        put(i).start()
    for i in range(len(chunks)):
        fetch(i).wait()
        put(i).start()
    for i in order:
        put(i).wait()


def copy_out(groups, mixed, tokens, own, sums, scale):
    any_spec = pl.BlockSpec(memory_space=pl.ANY)
    count = mixed.shape[0] // COPY_ROWS + 6
    return pl.pallas_call(
        functools.partial(copy_kernel, groups),
        in_specs=[any_spec] * 5,
        out_specs=any_spec,
        out_shape=jax.ShapeDtypeStruct(mixed.shape, mixed.dtype),
        scratch_shapes=[
            pltpu.VMEM(mixed.shape, mixed.dtype),
            pltpu.VMEM(own.shape, own.dtype),
            pltpu.VMEM(sums.shape, sums.dtype),
            pltpu.VMEM(scale.shape, scale.dtype),
            pltpu.SemaphoreType.DMA((count,)),
            pltpu.SemaphoreType.DMA((3,)),
            pltpu.SemaphoreType.DMA((count,)),
        ],
        compiler_params=pltpu.CompilerParams(vmem_limit_bytes=56 * 1024 * 1024),
    )(mixed, tokens, own, sums, scale)


def on_device(
    tokens, norm_gain, query_weight, key_weight, value_weight, out_weight, past_cache, exponents
):
    own_rows, depth = tokens.shape
    ranks = lax.axis_size("tensor")
    unit = 2 * PIECE
    batches = own_rows // unit
    units = ranks * batches
    q_cols = query_weight.shape[1]
    k_cols = key_weight.shape[1]
    kv_heads = k_cols // HD
    cache_len = past_cache.shape[1]
    cache_rows = SEQ_BLOCK * cache_len
    cosine, sine_part = rotary_tables(cache_len)
    bias = mask_table(cache_len)
    any_spec = pl.BlockSpec(memory_space=pl.ANY)
    bf16 = jnp.bfloat16
    dma = pltpu.SemaphoreType.DMA
    tail = (2, LAST[-1][1])
    mixed, own, sums, scale = pl.pallas_call(
        functools.partial(layer_kernel, ranks, batches),
        in_specs=[any_spec] * 11,
        out_specs=[any_spec] * 4,
        out_shape=[
            jax.ShapeDtypeStruct(tokens.shape, bf16),
            jax.ShapeDtypeStruct(tail + (depth,), bf16),
            jax.ShapeDtypeStruct(tail + (depth,), bf16),
            jax.ShapeDtypeStruct(tail + (128,), jnp.float32),
        ],
        scratch_shapes=[
            pltpu.VMEM((units + batches, unit, depth), bf16),
            pltpu.VMEM((units - batches, unit, depth), bf16),
            pltpu.VMEM((depth, q_cols), bf16),
            pltpu.VMEM((depth, k_cols), bf16),
            pltpu.VMEM((depth, k_cols), bf16),
            pltpu.VMEM((q_cols, depth), bf16),
            pltpu.VMEM((unit, q_cols), bf16),
            pltpu.VMEM((unit, k_cols), bf16),
            pltpu.VMEM((unit, k_cols), bf16),
            pltpu.VMEM((cache_rows + PIECE, HD), bf16),
            pltpu.VMEM((cache_rows + PIECE, HD), bf16),
            pltpu.VMEM((2 * kv_heads, SEQ_BLOCK, cache_len, 2, HD), bf16),
            pltpu.VMEM((cache_rows, HD), jnp.float32),
            pltpu.VMEM(norm_gain.shape, bf16),
            pltpu.VMEM(exponents.shape[::-1], jnp.int32),
            pltpu.VMEM(cosine.shape, jnp.float32),
            pltpu.VMEM(sine_part.shape, jnp.float32),
            pltpu.VMEM(bias.shape, jnp.float32),
            pltpu.VMEM((1, depth), jnp.float32),
            pltpu.VMEM((exponents.shape[0], 128), bf16),
            pltpu.VMEM((unit, 128), jnp.float32),
            dma((4,)),
            dma((5,)),
            dma((2, kv_heads)),
            dma((batches, 2, len(FIRST))),
            dma((batches, 2, len(LAST))),
            dma((2, 2)),
            dma((units - batches, 2)),
            dma((units - batches, 2)),
            dma((units - batches, 2)),
            dma((units - batches, 2)),
            dma((batches, 2, len(LAST))),
            dma((batches, 2, len(LAST))),
        ],
        compiler_params=pltpu.CompilerParams(
            collective_id=0, has_side_effects=True, vmem_limit_bytes=67043328
        ),
    )(
        tokens,
        norm_gain,
        query_weight,
        key_weight,
        value_weight,
        out_weight,
        past_cache,
        exponents.T,
        cosine,
        sine_part,
        bias,
    )
    return copy_out(exponents.shape[1], mixed, tokens, own, sums, scale)


def solution(mesh):
    return jax.shard_map(
        on_device,
        mesh=mesh,
        in_specs=(
            P(("dp", "tensor"), None),
            P(),
            P(None, "tensor"),
            P(None, "tensor"),
            P(None, "tensor"),
            P("tensor", None),
            P("dp", None, None, "tensor"),
            P("dp", None),
        ),
        out_specs=P(("dp", "tensor"), None),
        check_vma=False,
    )
```
